32 devices in a mesh: shot: 4 (over x, core), gx: 2 (over y), gy: 4 (over z).
Axes of the slice: x: 2, y: 2, z: 4, core: 2. Of those that a mesh axis runs over, the one named last changes fastest.
Arguments:
- state_now: float32 [4, 16, 256, 256], P('shot', 'gx', 'gy'), may hold values from -6 to 6
- state_prev: float32 [4, 16, 256, 256], P('shot', 'gx', 'gy'), may hold values from -6 to 6
- courant_sq: float32 [16, 256, 256], P('gx', 'gy'), may hold values from 0.03 to 0.3
- reflectivity: float32 [16, 256, 256], P('gx', 'gy'), may hold values from -6 to 6
- direction: float32 [16, 256, 256], P('gx', 'gy'), may hold values from -6 to 6
- prev_gradient: float32 [16, 256, 256], P('gx', 'gy'), may hold values from -3 to 3
- residual: float32 [4, 16, 16, 256], P('shot', None, 'gx', 'gy'), may hold values from -6 to 6
- rec_depth: int32 [4, 16, 256], P('shot', 'gx', 'gy'), may hold values from 0 to 255
- source_cell: int32 [4, 3], P('shot'), may hold values from 0 to 255, as said below
- wavelet: float32 [4, 15], P('shot'), may hold values from -80 to 80
- live_steps: int32 [4], P('shot'), may hold values from 8 to 16
Outputs:
- image_next: float32 [16, 256, 256], P('gx', 'gy')
- direction_next: float32 [16, 256, 256], P('gx', 'gy')
- residual_next: float32 [4, 16, 16, 256], P('shot', None, 'gx', 'gy')
- data_misfit: float32 [], replicated
The draws below stay inside these ranges and needn't reach their ends.
Inputs may be any that keep to these rules, and one draw needn't show every extreme that they name: `source_cell`: column 0 lies in 0 to 15, column 1 in 0 to 255, column 2 in 0 to 255.
All inputs are finite; a program needn't handle non-finite values.
Results may differ from the reference program's by a relative error of at most 0.0003.
Values sent between devices are 32-bit elements; how exact they have to be, the bound alone decides.
A program may use at most 64 MiB of HBM per device.

```python
import math
from functools import partial
import jax
import jax.numpy as jnp
from jax import lax

NT = 16
SHOTS = 4
NX = 16
NY = 256
NZ = 256


def draw_source_cell(key, part):
    keys = jax.random.split(jax.random.fold_in(key, 11), 3)
    first = jax.random.randint(keys[0], (SHOTS,), 0, NX)
    second = jax.random.randint(keys[1], (SHOTS,), 0, NY)
    third = jax.random.randint(keys[2], (SHOTS,), 0, NZ)
    return jnp.stack([first, second, third], axis=1).astype(jnp.int32)


def set_ends(array, key, least, top_value):
    dims = array.shape
    spot = [jax.random.randint(jax.random.fold_in(key, axis), (), 0, dims[axis]) for axis in range(len(dims))]
    array = array.at[tuple(spot)].set(least)
    longest = dims.index(max(dims))
    spot[longest] = (spot[longest] + 1) % dims[longest]
    return array.at[tuple(spot)].set(top_value)


def levels(own_key, extent, cuts, low, top_value):
    def one(dim, shards_of):
        heights = jax.random.uniform(jax.random.fold_in(jax.random.fold_in(own_key, 6), dim), (shards_of,), jnp.float32, low / len(cuts), top_value / len(cuts))
        return jnp.repeat(jnp.exp(heights), extent[dim] // shards_of).reshape((-1,) + (1,) * (len(extent) - dim - 1))

    level = one(*cuts[0])
    for cut in cuts[1:]:
        level = level * one(*cut)
    return level


def normal_values(key, dims, spread, bound, cuts=(), held_as=jnp.bfloat16):
    level = levels(key, dims, cuts, -0.22, 0.18) if cuts else 1.0
    values = jax.random.normal(key, dims, jnp.float32) * spread * level
    return jnp.minimum(jnp.maximum(values, -bound), bound).astype(held_as)


def setup_inputs(seed: int = 0) -> dict:
    streams_of = jax.random.split(jax.random.key(seed), 12)
    return {
        "state_now": normal_values(streams_of[0], (SHOTS, NX, NY, NZ), 1.0, 6.0, ((0, 4), (1, 2), (2, 4)), jnp.float32),
        "state_prev": normal_values(streams_of[1], (SHOTS, NX, NY, NZ), 1.0, 6.0, ((0, 4), (1, 2), (2, 4)), jnp.float32),
        "courant_sq": jnp.clip(jnp.exp(math.log(0.3) - 2.3025852 * jax.random.uniform(streams_of[2], (NX, NY, NZ), jnp.float32) ** levels(streams_of[2], (NX, NY, NZ), ((0, 2), (1, 4)), -0.2, 0.2)), 0.03, 0.3),
        "reflectivity": normal_values(streams_of[3], (NX, NY, NZ), 1.0, 6.0, ((0, 2), (1, 4)), jnp.float32),
        "direction": normal_values(streams_of[4], (NX, NY, NZ), 1.0, 6.0, ((0, 2), (1, 4)), jnp.float32),
        "prev_gradient": normal_values(streams_of[5], (NX, NY, NZ), 0.5, 3.0, ((0, 2), (1, 4)), jnp.float32),
        "residual": normal_values(streams_of[6], (SHOTS, NT, NX, NY), 1.0, 6.0, ((0, 4), (2, 2), (3, 4)), jnp.float32),
        "rec_depth": set_ends(jax.random.randint(streams_of[7], (SHOTS, NX, NY), 0, NZ), jax.random.fold_in(streams_of[7], 1), 0, NZ - 1).astype(jnp.int32),
        "source_cell": draw_source_cell(jax.random.fold_in(streams_of[11], 71), 0),
        "wavelet": normal_values(streams_of[9], (SHOTS, NT - 1), 20.0, 80.0, ((0, 4),), jnp.float32),
        "live_steps": set_ends(jax.random.randint(streams_of[10], (SHOTS,), NT // 2, NT + 1), jax.random.fold_in(streams_of[10], 1), NT // 2, NT).astype(jnp.int32),
    }


def laplace(values):
    padded = jnp.pad(values, 1)
    beside = padded[2:, 1:-1, 1:-1] + padded[:-2, 1:-1, 1:-1] + padded[1:-1, 2:, 1:-1] + padded[1:-1, :-2, 1:-1]
    beside = beside + padded[1:-1, 1:-1, 2:] + padded[1:-1, 1:-1, :-2]
    return beside - 6.0 * values


def background(courant_sq, start, before, amplitudes, cell):
    axis_x = jnp.arange(NX, dtype=jnp.int32)
    axis_y = jnp.arange(NY, dtype=jnp.int32)
    axis_z = jnp.arange(NZ, dtype=jnp.int32)
    spot = ((axis_x[:, None, None] == cell[0]) & (axis_y[None, :, None] == cell[1]) & (axis_z[None, None, :] == cell[2])).astype(jnp.float32)

    def advance(carry, amplitude):
        present, former = carry
        advanced = 2.0 * present - former + courant_sq * laplace(present) + amplitude * spot
        return (advanced, present), present

    (final_state, unused), history = lax.scan(advance, (start, before), amplitudes)
    return jnp.concatenate([history, final_state[None]], axis=0)


def receiver_mask(depth):
    axis_z = jnp.arange(NZ, dtype=jnp.int32)
    return (axis_z[None, None, :] == depth[:, :, None]).astype(jnp.float32)


def live_weights(count):
    return (jnp.arange(NT, dtype=jnp.int32) < count).astype(jnp.float32)


def shot_gradient(courant_sq, inputs):
    start, before, amplitudes, cell, depth, count, records = inputs
    stored = background(courant_sq, start, before, amplitudes, cell)
    mask = receiver_mask(depth)
    weighted = records * live_weights(count)[:, None, None]
    newest = mask * weighted[NT - 1][:, :, None]
    accumulated = stored[NT - 1] * newest

    def retreat(carry, pair):
        following, furthest, summed = carry
        weight, wavefield = pair
        scaled = courant_sq * following
        current = 2.0 * following - furthest + laplace(scaled) + mask * weight[:, :, None]
        return (current, following, summed + wavefield * current), None

    zeros = jnp.zeros_like(start)
    (unused_a, unused_b, accumulated), unused_c = lax.scan(retreat, (newest, zeros, accumulated), (weighted[:NT - 1], stored[:NT - 1]), reverse=True)
    return accumulated


def shot_records(courant_sq, gain, inputs):
    start, before, amplitudes, cell, depth, count = inputs
    stored = background(courant_sq, start, before, amplitudes, cell)
    mask = receiver_mask(depth)

    def advance(carry, wavefield):
        present, former = carry
        advanced = 2.0 * present - former + courant_sq * laplace(present) + gain * wavefield
        return (advanced, present), jnp.sum(mask * advanced, axis=2)

    zeros = jnp.zeros_like(start)
    unused, records = lax.scan(advance, (zeros, zeros), stored)
    return records * live_weights(count)[:, None, None]


def reference(state_now, state_prev, courant_sq, reflectivity, direction, prev_gradient, residual, rec_depth, source_cell, wavelet, live_steps):
    grads = lax.map(partial(shot_gradient, courant_sq), (state_now, state_prev, wavelet, source_cell, rec_depth, live_steps, residual))
    gradient = courant_sq * jnp.sum(grads, axis=0)
    grad_sq = jnp.sum(gradient * gradient)
    cross = jnp.sum(gradient * prev_gradient)
    old_sq = jnp.sum(prev_gradient * prev_gradient)
    beta_coef = (grad_sq - cross) / old_sq
    direction_next = gradient + beta_coef * direction
    slope = jnp.sum(gradient * direction_next)
    gain = courant_sq * direction_next
    records = lax.map(partial(shot_records, courant_sq, gain), (state_now, state_prev, wavelet, source_cell, rec_depth, live_steps))
    step_length = slope / jnp.sum(records * records)
    image_next = reflectivity + step_length * direction_next
    residual_next = residual - step_length * records
    data_misfit = 0.5 * jnp.mean(residual_next * residual_next)
    return image_next, direction_next, residual_next, data_misfit
```

```python
import functools

import jax
import jax.numpy as jnp
from jax import lax
from jax.experimental import pallas as pl
from jax.experimental.pallas import tpu as pltpu
from jax.sharding import PartitionSpec as P

MESH = pl.DeviceIdType.MESH
LANES = 128


def shifted(v, axis):
    size = v.shape[axis]
    index = lax.broadcasted_iota(jnp.int32, v.shape, axis)
    before = jnp.where(index == 0, 0.0, pltpu.roll(v, 1, axis))
    after = jnp.where(index == size - 1, 0.0, pltpu.roll(v, size - 1, axis))
    return before + after


def advance(below, present, above, former, speed):
    around = (below + above) + shifted(present, 0) + shifted(present, 1)
    return 2.0 * present - former + speed * (around - 6.0 * present)


def fold(v):
    return jnp.sum(v, axis=0, keepdims=True)


def lanes_folded(v):
    total = v[:, :LANES]
    for k in range(1, v.shape[1] // LANES):
        total = total + v[:, k * LANES:(k + 1) * LANES]
    return total


def kernel(
    sizes,
    cell_ref, wave_ref, now_ref, prev_ref, speed_ref, path_ref, old_ref, trace_ref, live_ref, rr_ref,
    dn_out, rec_out, stat_out, total_out,
    both, born, speed, path, old, trace, depth, grad, parts, reduced, gain, dn, dn_home, rec, rec_home,
    tile_a, slots_a, tile_b, slots_b,
    local_sem, home_send, home_recv, edge_send, edge_recv, born_send, born_recv,
    part_send, part_recv, share_send, share_recv, dn_send, dn_recv, rec_send, rec_recv,
    a_send, a_recv, b_send, b_recv,
):
    shots, across, along, steps = sizes
    shot, g, j = lax.axis_index("shot"), lax.axis_index("gx"), lax.axis_index("gy")
    block_y, extent_x, extent_z = now_ref.shape
    rows = block_y // across
    width = extent_x * across

    def snake(column, block):
        return jnp.where(lax.rem(block, 2) == 0, column, across - 1 - column)

    sigma = snake(g, j)
    place = j * across + sigma
    last = across * along - 1

    def chain(position):
        block = lax.div(position, across)
        return {"gx": snake(lax.rem(position, across), block), "gy": block}

    lower = chain(jnp.maximum(place - 1, 0))
    upper = chain(jnp.minimum(place + 1, last))

    targets = (
        (trace_ref, trace),
        (speed_ref, speed),
        (now_ref, both.at[1, pl.ds(1, rows), 0]),
        (prev_ref, both.at[0, pl.ds(1, rows), 0]),
        (path_ref, path),
        (old_ref, old),
    )
    mine = pl.ds(pl.multiple_of(g * extent_x, extent_x), extent_x)
    moves = []
    for k, (source, target) in enumerate(targets):
        own = pltpu.make_async_copy(
            source.at[pl.ds(sigma * rows, rows)], target.at[:, mine], local_sem.at[k]
        )
        own.start()
        group = [own]
        for d in range(1, across):
            peer = lax.rem(g + d, across)
            copy = pltpu.make_async_remote_copy(
                src_ref=source.at[pl.ds(snake(peer, j) * rows, rows)],
                dst_ref=target.at[:, mine],
                send_sem=home_send.at[k, d - 1],
                recv_sem=home_recv.at[k, d - 1],
                device_id={"gx": peer},
                device_id_type=MESH,
            )
            copy.start()
            group.append(copy)
        moves.append(group)

    flat = jnp.zeros((width, extent_z), jnp.float32)

    def clear(r, carry):
        both[0, r + 1, 1] = flat
        born[0, r + 1] = flat
        return carry

    lax.fori_loop(0, rows, clear, 0)
    rec[...] = jnp.zeros(rec.shape, jnp.float32)

    def clear_edge(row):
        def one(n, carry):
            both[n, row, 0] = flat
            both[n, row, 1] = flat
            born[n, row] = flat
            return carry

        lax.fori_loop(1, steps + 1, one, 0)

    @pl.when(place == 0)
    def _():
        clear_edge(0)

    @pl.when(place == last)
    def _():
        clear_edge(rows + 1)

    x_index = lax.broadcasted_iota(jnp.int32, (width, extent_z), 0)
    z_index = lax.broadcasted_iota(jnp.int32, (width, extent_z), 1)
    lane = lax.broadcasted_iota(jnp.int32, (width, LANES), 1)
    z_float = z_index.astype(jnp.float32)
    cell_x, cell_y, cell_z = cell_ref[0, 0], cell_ref[0, 1], cell_ref[0, 2]
    spot = jnp.where((x_index == cell_x) & (z_index == cell_z), 1.0, 0.0)
    first_row = j * block_y + sigma * rows

    def edges(field, n, sends, recvs):
        down = pltpu.make_async_remote_copy(
            src_ref=field.at[n, 1], dst_ref=field.at[n, rows + 1],
            send_sem=sends.at[n, 0], recv_sem=recvs.at[n, 0], device_id=lower, device_id_type=MESH,
        )
        up = pltpu.make_async_remote_copy(
            src_ref=field.at[n, rows], dst_ref=field.at[n, 0],
            send_sem=sends.at[n, 1], recv_sem=recvs.at[n, 1], device_id=upper, device_id_type=MESH,
        )
        return down, up

    def send_edges(field, n, sends, recvs):
        down, up = edges(field, n, sends, recvs)

        @pl.when(place > 0)
        def _():
            down.start()

        @pl.when(place < last)
        def _():
            up.start()

    def wait_edges(field, n, sends, recvs):
        down, up = edges(field, n, sends, recvs)

        @pl.when(place < last)
        def _():
            down.wait_recv()
            up.wait_send()

        @pl.when(place > 0)
        def _():
            up.wait_recv()
            down.wait_send()

    def picked(r, n):
        return jnp.sum(jnp.where(lane == n, trace[r], 0.0), axis=1, keepdims=True)

    def receivers(r):
        level = jnp.concatenate([depth[r]] * (extent_z // LANES), axis=1)
        return level == z_float

    unroll = 1
    for candidate in (2, 3):
        if (rows - 2) % candidate == 0:
            unroll = candidate

    for copy in moves[0]:
        copy.wait()
    for copy in moves[1]:
        copy.wait()

    def adjoint_start(r, carry):
        depth[r] = jnp.broadcast_to(picked(r, steps), (width, LANES))
        weight = picked(r, steps - 1)
        both[1, r + 1, 1] = jnp.where(receivers(r), speed[r] * weight, 0.0)
        return carry

    lax.fori_loop(0, rows, adjoint_start, 0)
    for k in (2, 3):
        for copy in moves[k]:
            copy.wait()
    send_edges(both, 1, edge_send, edge_recv)

    def forward_row(n, r):
        c = speed[r]
        amplitude = jnp.where(first_row + r == cell_y, wave_ref[0, n - 1], 0.0)
        u = advance(both[n, r, 0], both[n, r + 1, 0], both[n, r + 2, 0], both[n - 1, r + 1, 0], c)
        both[n + 1, r + 1, 0] = u + amplitude * spot
        v = advance(both[n, r, 1], both[n, r + 1, 1], both[n, r + 2, 1], both[n - 1, r + 1, 1], c)
        both[n + 1, r + 1, 1] = v + jnp.where(receivers(r), c * picked(r, steps - 1 - n), 0.0)

    def sweep(row_of, n):
        def one(r, carry):
            row_of(n, r)
            return carry

        lax.fori_loop(1, rows - 1, one, 0, unroll=unroll)

    def forward(n, carry):
        sweep(forward_row, n)
        wait_edges(both, n, edge_send, edge_recv)
        forward_row(n, 0)
        forward_row(n, rows - 1)

        @pl.when(n < steps - 1)
        def _():
            send_edges(both, n + 1, edge_send, edge_recv)

        return carry

    lax.fori_loop(1, steps, forward, 0)

    def image_row(r, carry):
        total = both[1, r + 1, 0] * both[steps, r + 1, 1]
        for a in range(2, steps + 1):
            total = total + both[a, r + 1, 0] * both[steps + 1 - a, r + 1, 1]
        grad[r] = total
        return carry

    lax.fori_loop(0, rows, image_row, 0)
    share = rows // shots
    copies = []
    for d in range(1, shots):
        peer = lax.rem(shot + d, shots)
        copy = pltpu.make_async_remote_copy(
            src_ref=grad.at[pl.ds(peer * share, share)], dst_ref=parts.at[d - 1],
            send_sem=part_send.at[d - 1], recv_sem=part_recv.at[d - 1],
            device_id={"shot": peer}, device_id_type=MESH,
        )
        copy.start()
        copies.append(copy)
    for copy in copies:
        copy.wait()
    own_share = shot * share

    def add_share(r, carry):
        total = grad[own_share + r]
        for d in range(1, shots):
            total = total + parts[d - 1, r]
        reduced[own_share + r] = total
        return carry

    lax.fori_loop(0, share, add_share, 0)
    copies = []
    for d in range(1, shots):
        peer = lax.rem(shot + d, shots)
        copy = pltpu.make_async_remote_copy(
            src_ref=reduced.at[pl.ds(own_share, share)], dst_ref=reduced.at[pl.ds(own_share, share)],
            send_sem=share_send.at[d - 1], recv_sem=share_recv.at[d - 1],
            device_id={"shot": peer}, device_id_type=MESH,
        )
        copy.start()
        copies.append(copy)
    for k in (4, 5):
        for copy in moves[k]:
            copy.wait()
    for copy in copies:
        copy.wait()

    zero = jnp.zeros((width, LANES), jnp.float32)

    def inner(r, carry):
        new, was, way = reduced[r], old[r], path[r]
        return (
            carry[0] + lanes_folded(new * new),
            carry[1] + lanes_folded(new * was),
            carry[2] + lanes_folded(was * was),
            carry[3] + lanes_folded(new * way),
        )

    sums = lax.fori_loop(0, rows, inner, (zero, zero, zero, zero))

    def write_tile(tile, values):
        tile[...] = jnp.concatenate(
            [fold(v) for v in values] + [jnp.zeros((8 - len(values), LANES), jnp.float32)], axis=0
        )

    def all_sum(tile, slots, count, rank, device_of, sends, recvs):
        copies = []
        for d in range(1, count):
            copy = pltpu.make_async_remote_copy(
                src_ref=tile, dst_ref=slots.at[rank],
                send_sem=sends.at[d - 1], recv_sem=recvs.at[d - 1],
                device_id=device_of(lax.rem(rank + d, count)), device_id_type=MESH,
            )
            copy.start()
            copies.append(copy)
        slots[rank] = tile[...]
        for copy in copies:
            copy.wait()
        return lax.fori_loop(0, count, lambda k, total: total + slots[k], jnp.zeros((8, LANES), jnp.float32))

    grid_rank = g * along + j
    write_tile(tile_a, sums)
    stats = all_sum(
        tile_a, slots_a, across * along, grid_rank,
        lambda k: {"gx": lax.div(k, along), "gy": lax.rem(k, along)}, a_send, a_recv,
    )
    stat_out[...] = stats
    values = jnp.sum(stats, axis=1, keepdims=True)
    beta = (values[0:1] - values[1:2]) / values[2:3]

    def search(r, carry):
        new = reduced[r] + beta * path[r]
        dn[r] = new
        lift = speed[r] * new
        gain[r] = lift
        born[1, r + 1] = lift * both[1, r + 1, 0]
        return carry

    lax.fori_loop(0, rows, search, 0)
    send_edges(born, 1, born_send, born_recv)

    def homeward(field, home, sends, recvs):
        strip = pl.ds(sigma * rows, rows)
        copies = []
        for d in range(1, across):
            peer = lax.rem(g + d, across)
            part = pl.ds(pl.multiple_of(peer * extent_x, extent_x), extent_x)
            copies.append(pltpu.make_async_remote_copy(
                src_ref=field.at[:, part], dst_ref=home.at[strip],
                send_sem=sends.at[d], recv_sem=recvs.at[d - 1],
                device_id={"gx": peer}, device_id_type=MESH,
            ))
        copies.append(pltpu.make_async_copy(field.at[:, mine], home.at[strip], sends.at[0]))
        for copy in copies:
            copy.start()
        return copies

    def sample(n, r, w):
        hit = jnp.sum(jnp.where(receivers(r), w, 0.0), axis=1, keepdims=True)
        rec[r] = jnp.where(lane == n - 1, hit, rec[r])

    def first_sample(r, carry):
        sample(1, r, born[1, r + 1])
        return carry

    lax.fori_loop(0, rows, first_sample, 0)

    def born_row(n, r):
        w = advance(born[n, r], born[n, r + 1], born[n, r + 2], born[n - 1, r + 1], speed[r])
        w = w + gain[r] * both[n + 1, r + 1, 0]
        born[n + 1, r + 1] = w
        sample(n + 1, r, w)

    def scatter(n, carry):
        sweep(born_row, n)
        wait_edges(born, n, born_send, born_recv)
        born_row(n, 0)
        born_row(n, rows - 1)

        @pl.when(n < steps - 1)
        def _():
            send_edges(born, n + 1, born_send, born_recv)

        return carry

    lax.fori_loop(1, steps, scatter, 0)
    dn_moves = homeward(dn, dn_home, dn_send, dn_recv)

    def finish(r, carry):
        row = rec[r] * live_ref[0:1]
        rec[r] = row
        return carry[0] + row * row, carry[1] + trace[r] * row

    sums = lax.fori_loop(0, rows, finish, (zero, zero))
    write_tile(tile_b, sums + (rr_ref[...],))
    rec_moves = homeward(rec, rec_home, rec_send, rec_recv)
    grid = across * along
    total_out[...] = all_sum(
        tile_b, slots_b, shots * grid, shot * grid + grid_rank,
        lambda k: {
            "shot": lax.div(k, grid),
            "gx": lax.div(lax.rem(k, grid), along),
            "gy": lax.rem(k, along),
        },
        b_send, b_recv,
    )
    for copy in dn_moves + rec_moves:
        copy.wait()
    dn_out[...] = dn_home[...]
    rec_out[...] = rec_home[...]


def on_device(
    state_now, state_prev, courant_sq, reflectivity, direction, prev_gradient,
    residual, rec_depth, source_cell, wavelet, live_steps,
):
    shots, across, along = (lax.axis_size(a) for a in ("shot", "gx", "gy"))
    steps = residual.shape[1]
    extent_x, block_y, extent_z = courant_sq.shape
    rows, width = block_y // across, extent_x * across

    def turned(v):
        return jnp.transpose(v, (1, 0, 2))

    live = (lax.iota(jnp.int32, steps) < live_steps[0]).astype(jnp.float32)
    weighted = residual[0] * live[:, None, None]
    packed = jnp.concatenate([weighted, rec_depth.astype(jnp.float32)], axis=0)
    packed = jnp.pad(jnp.transpose(packed, (2, 1, 0)), ((0, 0), (0, 0), (0, LANES - steps - 1)))
    live_lanes = jnp.broadcast_to(jnp.pad(live, (0, LANES - steps)), (8, LANES))
    squares = jnp.sum(residual * residual)
    rr = jnp.pad(squares.reshape(1, 1), ((0, 7), (0, LANES - 1)))

    f32 = jnp.float32
    strip = (rows, width, extent_z)
    home = (block_y, extent_x, extent_z)
    grid = across * along
    dma = pltpu.SemaphoreType.DMA
    one = max(across - 1, 1)
    scratch = [
        pltpu.VMEM((steps + 1, rows + 2, 2, width, extent_z), f32),
        pltpu.VMEM((steps + 1, rows + 2, width, extent_z), f32),
        pltpu.VMEM(strip, f32),
        pltpu.VMEM(strip, f32),
        pltpu.VMEM(strip, f32),
        pltpu.VMEM((rows, width, LANES), f32),
        pltpu.VMEM((rows, width, LANES), f32),
        pltpu.VMEM(strip, f32),
        pltpu.VMEM((shots - 1, rows // shots, width, extent_z), f32),
        pltpu.VMEM(strip, f32),
        pltpu.VMEM(strip, f32),
        pltpu.VMEM(strip, f32),
        pltpu.VMEM(home, f32),
        pltpu.VMEM((rows, width, LANES), f32),
        pltpu.VMEM((block_y, extent_x, LANES), f32),
        pltpu.VMEM((8, LANES), f32),
        pltpu.VMEM((grid, 8, LANES), f32),
        pltpu.VMEM((8, LANES), f32),
        pltpu.VMEM((shots * grid, 8, LANES), f32),
        dma((6,)), dma((6, one)), dma((6, one)),
        dma((steps + 1, 2)), dma((steps + 1, 2)), dma((steps + 1, 2)), dma((steps + 1, 2)),
        dma((shots - 1,)), dma((shots - 1,)), dma((shots - 1,)), dma((shots - 1,)),
        dma((across,)), dma((one,)), dma((across,)), dma((one,)),
        dma((grid - 1,)), dma((grid - 1,)), dma((shots * grid - 1,)), dma((shots * grid - 1,)),
    ]
    vmem, smem = pl.BlockSpec(memory_space=pltpu.VMEM), pl.BlockSpec(memory_space=pltpu.SMEM)
    dn, rec, stats, totals = pl.pallas_call(
        functools.partial(kernel, (shots, across, along, steps)),
        out_shape=(
            jax.ShapeDtypeStruct(home, f32),
            jax.ShapeDtypeStruct((block_y, extent_x, LANES), f32),
            jax.ShapeDtypeStruct((8, LANES), f32),
            jax.ShapeDtypeStruct((8, LANES), f32),
        ),
        in_specs=[smem, smem] + [vmem] * 8,
        out_specs=(vmem,) * 4,
        scratch_shapes=scratch,
        compiler_params=pltpu.CompilerParams(has_side_effects=True, vmem_limit_bytes=60 * 1024 * 1024),
        name="iteration",
    )(
        source_cell, wavelet, turned(state_now[0]), turned(state_prev[0]), turned(courant_sq),
        turned(direction), turned(prev_gradient), packed, live_lanes, rr,
    )
    sums = jnp.sum(stats, axis=1)
    ends = jnp.sum(totals, axis=1)
    beta = (sums[0] - sums[1]) / sums[2]
    slope = sums[0] + beta * sums[3]
    step = slope / ends[0]
    direction_next = turned(dn)
    image_next = reflectivity + step * direction_next
    records = jnp.transpose(rec[:, :, :steps], (2, 1, 0))
    residual_next = residual - step * records[None]
    entries = float(residual.size * shots * grid)
    misfit = ends[2] - 2.0 * step * ends[1] + step * step * ends[0]
    return image_next, direction_next, residual_next, 0.5 * misfit / entries


def solution(mesh):
    field, flat = P("shot", "gx", "gy", None), P("gx", "gy", None)
    traces = P("shot", None, "gx", "gy")
    return jax.shard_map(
        on_device,
        mesh=mesh,
        in_specs=(
            field, field, flat, flat, flat, flat, traces,
            P("shot", "gx", "gy"), P("shot", None), P("shot", None), P("shot"),
        ),
        out_specs=(flat, flat, traces, P()),
        check_vma=False,
    )
```

```python
import functools

import jax
import jax.numpy as jnp
from jax import lax
from jax.experimental import pallas as pl
from jax.experimental.pallas import tpu as pltpu
from jax.sharding import PartitionSpec as P

MESH = pl.DeviceIdType.MESH
LANES = 128


def shifted(v, axis):
    size = v.shape[axis]
    index = lax.broadcasted_iota(jnp.int32, v.shape, axis)
    before = jnp.where(index == 0, 0.0, pltpu.roll(v, 1, axis))
    after = jnp.where(index == size - 1, 0.0, pltpu.roll(v, size - 1, axis))
    return before + after


def advance(below, present, above, former, speed):
    around = (below + above) + shifted(present, 0) + shifted(present, 1)
    return 2.0 * present - former + speed * (around - 6.0 * present)


def fold(v):
    return jnp.sum(v, axis=0, keepdims=True)


def lanes_folded(v):
    total = v[:, :LANES]
    for k in range(1, v.shape[1] // LANES):
        total = total + v[:, k * LANES:(k + 1) * LANES]
    return total


def kernel(
    sizes,
    cell_ref, wave_ref, now_ref, prev_ref, speed_ref, path_ref, old_ref, trace_ref, live_ref, rr_ref,
    dn_out, rec_out, stat_out, total_out,
    both, born, speed, path, old, trace, depth, grad, parts, reduced, gain, dn, dn_home, rec, rec_home,
    tile_a, slots_a, tile_b, slots_b,
    local_sem, home_send, home_recv, later_send, later_recv, edge_send, edge_recv, born_send, born_recv, once_send, once_recv,
    part_send, part_recv, share_send, share_recv, dn_send, dn_recv, rec_send, rec_recv,
    a_send, a_recv, b_send, b_recv,
):
    shots, across, along, steps, fit, chunks = sizes
    shot, g, j = lax.axis_index("shot"), lax.axis_index("gx"), lax.axis_index("gy")
    block_y, extent_x, extent_z = now_ref.shape
    rows = block_y // across
    width = extent_x * across
    size = rows // chunks

    def snake(column, block):
        return jnp.where(lax.rem(block, 2) == 0, column, across - 1 - column)

    sigma = snake(g, j)
    place = j * across + sigma
    last = across * along - 1

    def chain(position):
        block = lax.div(position, across)
        return {"gx": snake(lax.rem(position, across), block), "gy": block}

    lower = chain(jnp.maximum(place - 1, 0))
    upper = chain(jnp.minimum(place + 1, last))

    targets = (
        (trace_ref, trace.at[pl.ds(1, rows // fit)]),
        (speed_ref, speed.at[pl.ds(1, rows)]),
        (now_ref, both.at[1, pl.ds(2, rows), 0]),
        (prev_ref, both.at[0, pl.ds(2, rows), 0]),
    )
    later = ((path_ref, path), (old_ref, old))
    mine = pl.ds(pl.multiple_of(g * extent_x, extent_x), extent_x)
    moves = []
    for k, (source, target) in enumerate(targets):
        count = target.shape[0]
        own = pltpu.make_async_copy(
            source.at[pl.ds(sigma * count, count)], target.at[:, mine], local_sem.at[k]
        )
        own.start()
        group = [own]
        for d in range(1, across):
            peer = lax.rem(g + d, across)
            copy = pltpu.make_async_remote_copy(
                src_ref=source.at[pl.ds(snake(peer, j) * count, count)],
                dst_ref=target.at[:, mine],
                send_sem=home_send.at[k, d - 1],
                recv_sem=home_recv.at[k, d - 1],
                device_id={"gx": peer},
                device_id_type=MESH,
            )
            copy.start()
            group.append(copy)
        moves.append(group)
    own_later = []
    for k, (source, target) in enumerate(later):
        own = pltpu.make_async_copy(
            source.at[pl.ds(sigma * rows, rows)], target.at[:, mine], local_sem.at[len(targets) + k]
        )
        own.start()
        own_later.append(own)

    def later_copies(k, e):
        source, target = later[k]
        copies = []
        for d in range(1, across):
            peer = lax.rem(g + d, across)
            copies.append(pltpu.make_async_remote_copy(
                src_ref=source.at[pl.ds(snake(peer, j) * rows + e * size, size)],
                dst_ref=target.at[pl.ds(e * size, size), mine],
                send_sem=later_send.at[k, d - 1, e], recv_sem=later_recv.at[k, d - 1, e],
                device_id={"gx": peer}, device_id_type=MESH,
            ))
        return copies

    flat = jnp.zeros((width, extent_z), jnp.float32)

    def clear(r, carry):
        both[0, r, 1] = flat
        born[0, r] = flat
        return carry

    lax.fori_loop(0, rows + 4, clear, 0)
    rec[...] = jnp.zeros(rec.shape, jnp.float32)

    def clear_edge(first, single, line):
        def one(n, carry):
            for row in (first, first + 1):
                both[n, row, 0] = flat
                both[n, row, 1] = flat
                born[n, row] = flat
            return carry

        lax.fori_loop(0, steps + 1, one, 0)
        speed[single] = flat
        gain[single] = flat
        trace[line] = flat[:, :LANES]

    @pl.when(place == 0)
    def _():
        clear_edge(0, 0, 0)

    @pl.when(place == last)
    def _():
        clear_edge(rows + 2, rows + 1, rows // fit + 1)

    x_index = lax.broadcasted_iota(jnp.int32, (width, extent_z), 0)
    z_index = lax.broadcasted_iota(jnp.int32, (width, extent_z), 1)
    lane = lax.broadcasted_iota(jnp.int32, (width, LANES), 1)
    z_float = z_index.astype(jnp.float32)
    cell_x, cell_y, cell_z = cell_ref[0, 0], cell_ref[0, 1], cell_ref[0, 2]
    spot = jnp.where((x_index == cell_x) & (z_index == cell_z), 1.0, 0.0)
    first_row = j * block_y + sigma * rows

    def pair(view, own, pad, deep, sends, recvs, k):
        down = pltpu.make_async_remote_copy(
            src_ref=view(pad, deep), dst_ref=view(pad + own, deep),
            send_sem=sends.at[k, 0], recv_sem=recvs.at[k, 0], device_id=lower, device_id_type=MESH,
        )
        up = pltpu.make_async_remote_copy(
            src_ref=view(pad + own - deep, deep), dst_ref=view(pad - deep, deep),
            send_sem=sends.at[k, 1], recv_sem=recvs.at[k, 1], device_id=upper, device_id_type=MESH,
        )
        return down, up

    def both_edges(n):
        return pair(lambda a, c: both.at[n, pl.ds(a, c)], rows, 2, 2, edge_send, edge_recv, n)

    def born_edges(n):
        return pair(lambda a, c: born.at[n, pl.ds(a, c)], rows, 2, 2, born_send, born_recv, n)

    def once_edges(k):
        if k == 0:
            return pair(lambda a, c: trace.at[pl.ds(a, c)], rows // fit, 1, 1, once_send, once_recv, k)
        if k == 2:
            return pair(lambda a, c: both.at[0, pl.ds(a, c), 0], rows, 2, 1, once_send, once_recv, k)
        field = speed if k == 1 else gain
        return pair(lambda a, c: field.at[pl.ds(a, c)], rows, 1, 1, once_send, once_recv, k)

    def send_edges(copies):
        @pl.when(place > 0)
        def _():
            copies[0].start()

        @pl.when(place < last)
        def _():
            copies[1].start()

    def wait_edges(copies):
        @pl.when(place < last)
        def _():
            copies[0].wait_recv()
            copies[1].wait_send()

        @pl.when(place > 0)
        def _():
            copies[1].wait_recv()
            copies[0].wait_send()

    def place_of(r, n):
        line = r // fit if isinstance(r, int) else lax.div(r, fit)
        return line, lane == (r - line * fit) * (LANES // fit) + n

    def picked(r, n):
        line, chosen = place_of(r + fit, n)
        return jnp.sum(jnp.where(chosen, trace[line], 0.0), axis=1, keepdims=True)

    def receivers(r):
        level = jnp.concatenate([depth[r + 1]] * (extent_z // LANES), axis=1)
        return level == z_float

    def inside(r, v):
        if isinstance(r, int) and r < 0:
            return jnp.where(place > 0, v, 0.0)
        if isinstance(r, int) and r >= rows:
            return jnp.where(place < last, v, 0.0)
        return v

    def together(ops, n, where):
        values = [ops[0](n, r) for r in where]
        for r, value in zip(where, values):
            ops[1](n, r, value)

    def sweep(ops, n, first, count):
        group = 1
        for candidate in (2, 3):
            if count % candidate == 0:
                group = candidate

        def one(i, carry):
            together(ops, n, [first + i * group + k for k in range(group)])
            return carry

        lax.fori_loop(0, count // group, one, 0)

    rounds = (steps - 1) // 2

    def march(ops, edges_of, before_edges, after_send):
        def step_pair(i, carry):
            n = 1 + 2 * i
            sweep(ops, n, 1, rows - 2)
            sweep(ops, n + 1, 2, rows - 4)
            wait_edges(edges_of(n))

            @pl.when(i == 0)
            def _():
                before_edges()

            together(ops, n, [-1, 0, rows - 1, rows])
            together(ops, n + 1, [0, 1, rows - 2, rows - 1])

            @pl.when(n + 2 < steps)
            def _():
                send_edges(edges_of(n + 2))

            after_send(i)
            return carry

        lax.fori_loop(0, rounds, step_pair, 0)
        if (steps - 1) % 2:
            sweep(ops, steps - 1, 1, rows - 2)
            wait_edges(edges_of(steps - 1))
            together(ops, steps - 1, [0, rows - 1])

    for copy in moves[0]:
        copy.wait()
    for copy in moves[1]:
        copy.wait()

    for k in (0, 1):
        send_edges(once_edges(k))

    def adjoint_start(r, carry):
        depth[r + 1] = jnp.broadcast_to(picked(r, steps), (width, LANES))
        weight = picked(r, steps - 1)
        both[1, r + 2, 1] = jnp.where(receivers(r), speed[r + 1] * weight, 0.0)
        return carry

    lax.fori_loop(0, rows, adjoint_start, 0)
    for k in (2, 3):
        for copy in moves[k]:
            copy.wait()
    send_edges(both_edges(1))
    send_edges(once_edges(2))

    def forward_value(n, r):
        c = speed[r + 1]
        amplitude = jnp.where(first_row + r == cell_y, wave_ref[0, n - 1], 0.0)
        u = advance(both[n, r + 1, 0], both[n, r + 2, 0], both[n, r + 3, 0], both[n - 1, r + 2, 0], c)
        v = advance(both[n, r + 1, 1], both[n, r + 2, 1], both[n, r + 3, 1], both[n - 1, r + 2, 1], c)
        v = v + jnp.where(receivers(r), c * picked(r, steps - 1 - n), 0.0)
        return inside(r, u + amplitude * spot), inside(r, v)

    def forward_put(n, r, value):
        both[n + 1, r + 2, 0], both[n + 1, r + 2, 1] = value

    def first_halos():
        for k in (0, 1, 2):
            wait_edges(once_edges(k))
        for r in (-1, rows):
            depth[r + 1] = jnp.broadcast_to(picked(r, steps), (width, LANES))

    def regroup_later(i):
        for k, offset in ((0, 0), (1, rounds - chunks)):
            @pl.when((i >= offset) & (i < offset + chunks))
            def _():
                for copy in later_copies(k, i - offset):
                    copy.start()

    march((forward_value, forward_put), both_edges, first_halos, regroup_later)

    def image_row(r, carry):
        total = both[1, r + 2, 0] * both[steps, r + 2, 1]
        for a in range(2, steps + 1):
            total = total + both[a, r + 2, 0] * both[steps + 1 - a, r + 2, 1]
        grad[r] = total
        return carry

    lax.fori_loop(0, rows, image_row, 0)
    share = rows // shots
    copies = []
    for d in range(1, shots):
        peer = lax.rem(shot + d, shots)
        copy = pltpu.make_async_remote_copy(
            src_ref=grad.at[pl.ds(peer * share, share)], dst_ref=parts.at[d - 1],
            send_sem=part_send.at[d - 1], recv_sem=part_recv.at[d - 1],
            device_id={"shot": peer}, device_id_type=MESH,
        )
        copy.start()
        copies.append(copy)
    for copy in copies:
        copy.wait()
    own_share = shot * share

    def add_share(r, carry):
        total = grad[own_share + r]
        for d in range(1, shots):
            total = total + parts[d - 1, r]
        reduced[own_share + r] = total
        return carry

    lax.fori_loop(0, share, add_share, 0)
    copies = []
    for d in range(1, shots):
        peer = lax.rem(shot + d, shots)
        copy = pltpu.make_async_remote_copy(
            src_ref=reduced.at[pl.ds(own_share, share)], dst_ref=reduced.at[pl.ds(own_share, share)],
            send_sem=share_send.at[d - 1], recv_sem=share_recv.at[d - 1],
            device_id={"shot": peer}, device_id_type=MESH,
        )
        copy.start()
        copies.append(copy)
    for copy in own_later:
        copy.wait()

    def later_wait(e, carry):
        for copy in later_copies(0, e) + later_copies(1, e):
            copy.wait()
        return carry

    lax.fori_loop(0, chunks, later_wait, 0)
    for copy in copies:
        copy.wait()

    zero = jnp.zeros((width, LANES), jnp.float32)

    def inner(r, carry):
        new, was, way = reduced[r], old[r], path[r]
        return (
            carry[0] + lanes_folded(new * new),
            carry[1] + lanes_folded(new * was),
            carry[2] + lanes_folded(was * was),
            carry[3] + lanes_folded(new * way),
        )

    sums = lax.fori_loop(0, rows, inner, (zero, zero, zero, zero))

    def write_tile(tile, values):
        tile[...] = jnp.concatenate(
            [fold(v) for v in values] + [jnp.zeros((8 - len(values), LANES), jnp.float32)], axis=0
        )

    def all_sum(tile, slots, count, rank, device_of, sends, recvs):
        copies = []
        for d in range(1, count):
            copy = pltpu.make_async_remote_copy(
                src_ref=tile, dst_ref=slots.at[rank],
                send_sem=sends.at[d - 1], recv_sem=recvs.at[d - 1],
                device_id=device_of(lax.rem(rank + d, count)), device_id_type=MESH,
            )
            copy.start()
            copies.append(copy)
        slots[rank] = tile[...]
        for copy in copies:
            copy.wait()
        return lax.fori_loop(0, count, lambda k, total: total + slots[k], jnp.zeros((8, LANES), jnp.float32))

    grid_rank = g * along + j
    write_tile(tile_a, sums)
    stats = all_sum(
        tile_a, slots_a, across * along, grid_rank,
        lambda k: {"gx": lax.div(k, along), "gy": lax.rem(k, along)}, a_send, a_recv,
    )
    stat_out[...] = stats
    values = jnp.sum(stats, axis=1, keepdims=True)
    beta = (values[0:1] - values[1:2]) / values[2:3]

    def search(r, carry):
        new = reduced[r] + beta * path[r]
        dn[r] = new
        lift = speed[r + 1] * new
        gain[r + 1] = lift
        born[1, r + 2] = lift * both[1, r + 2, 0]
        return carry

    lax.fori_loop(0, rows, search, 0)
    send_edges(once_edges(3))
    send_edges(born_edges(1))

    def homeward(field, home, first, count, send_of, recv_of):
        copies = []
        for d in range(1, across):
            peer = lax.rem(g + d, across)
            part = pl.ds(pl.multiple_of(peer * extent_x, extent_x), extent_x)
            copies.append(pltpu.make_async_remote_copy(
                src_ref=field.at[pl.ds(first, count), part],
                dst_ref=home.at[pl.ds(sigma * field.shape[0] + first, count)],
                send_sem=send_of(d), recv_sem=recv_of(d - 1),
                device_id={"gx": peer}, device_id_type=MESH,
            ))
        copies.append(pltpu.make_async_copy(
            field.at[pl.ds(first, count), mine],
            home.at[pl.ds(sigma * field.shape[0] + first, count)], send_of(0),
        ))
        return copies

    def dn_copies(e):
        return homeward(
            dn, dn_home, e * size, size, lambda d: dn_send.at[d, e], lambda d: dn_recv.at[d, e]
        )

    def hit_of(r, w):
        return jnp.sum(jnp.where(receivers(r), w, 0.0), axis=1, keepdims=True)

    def sample(n, r, hit):
        line, chosen = place_of(r, n - 1)
        rec[line] = jnp.where(chosen, hit, rec[line])

    def first_sample(r, carry):
        sample(1, r, hit_of(r, born[1, r + 2]))
        return carry

    lax.fori_loop(0, rows, first_sample, 0)

    def born_value(n, r):
        w = advance(born[n, r + 1], born[n, r + 2], born[n, r + 3], born[n - 1, r + 2], speed[r + 1])
        w = inside(r, w + gain[r + 1] * both[n + 1, r + 2, 0])
        if isinstance(r, int) and not 0 <= r < rows:
            return w, None
        return w, hit_of(r, w)

    def born_put(n, r, value):
        born[n + 1, r + 2] = value[0]
        if value[1] is not None:
            sample(n + 1, r, value[1])

    def return_dn(i):
        @pl.when(i < chunks)
        def _():
            for copy in dn_copies(i):
                copy.start()

    march((born_value, born_put), born_edges, lambda: wait_edges(once_edges(3)), return_dn)

    def finish(r, carry):
        row = rec[r] * live_ref[0:1]
        rec[r] = row
        return carry[0] + row * row, carry[1] + trace[r + 1] * row

    sums = lax.fori_loop(0, rows // fit, finish, (zero, zero))
    write_tile(tile_b, sums + (rr_ref[...],))
    rec_moves = homeward(
        rec, rec_home, 0, rows // fit, lambda d: rec_send.at[d], lambda d: rec_recv.at[d]
    )
    for copy in rec_moves:
        copy.start()
    grid = across * along
    total_out[...] = all_sum(
        tile_b, slots_b, shots * grid, shot * grid + grid_rank,
        lambda k: {
            "shot": lax.div(k, grid),
            "gx": lax.div(lax.rem(k, grid), along),
            "gy": lax.rem(k, along),
        },
        b_send, b_recv,
    )
    def dn_wait(e, carry):
        for copy in dn_copies(e):
            copy.wait()
        return carry

    lax.fori_loop(0, chunks, dn_wait, 0)
    for copy in rec_moves:
        copy.wait()
    dn_out[...] = dn_home[...]
    rec_out[...] = rec_home[...]


def on_device(
    state_now, state_prev, courant_sq, reflectivity, direction, prev_gradient,
    residual, rec_depth, source_cell, wavelet, live_steps,
):
    shots, across, along = (lax.axis_size(a) for a in ("shot", "gx", "gy"))
    steps = residual.shape[1]
    extent_x, block_y, extent_z = courant_sq.shape
    rows, width = block_y // across, extent_x * across

    def turned(v):
        return jnp.transpose(v, (1, 0, 2))

    live = (lax.iota(jnp.int32, steps) < live_steps[0]).astype(jnp.float32)
    weighted = residual[0] * live[:, None, None]
    packed = jnp.concatenate([weighted, rec_depth.astype(jnp.float32)], axis=0)
    fit = 1
    while LANES // (2 * fit) > steps and rows % (2 * fit) == 0:
        fit *= 2
    pitch = LANES // fit
    chunks = rows
    while chunks > (steps - 1) // 2:
        chunks //= 2

    def gathered(v):
        v = jnp.pad(v, ((0, pitch - v.shape[0]), (0, 0), (0, 0)))
        v = v.reshape(pitch, extent_x, block_y // fit, fit)
        return jnp.transpose(v, (2, 1, 3, 0)).reshape(block_y // fit, extent_x, LANES)

    packed = gathered(packed)
    live_lanes = jnp.broadcast_to(jnp.tile(jnp.pad(live, (0, pitch - steps)), fit), (8, LANES))
    squares = jnp.sum(residual * residual)
    rr = jnp.pad(squares.reshape(1, 1), ((0, 7), (0, LANES - 1)))

    f32 = jnp.float32
    strip = (rows, width, extent_z)
    home = (block_y, extent_x, extent_z)
    grid = across * along
    dma = pltpu.SemaphoreType.DMA
    one = max(across - 1, 1)
    scratch = [
        pltpu.VMEM((steps + 1, rows + 4, 2, width, extent_z), f32),
        pltpu.VMEM((steps + 1, rows + 4, width, extent_z), f32),
        pltpu.VMEM((rows + 2, width, extent_z), f32),
        pltpu.VMEM(strip, f32),
        pltpu.VMEM(strip, f32),
        pltpu.VMEM((rows // fit + 2, width, LANES), f32),
        pltpu.VMEM((rows + 2, width, LANES), f32),
        pltpu.VMEM(strip, f32),
        pltpu.VMEM((shots - 1, rows // shots, width, extent_z), f32),
        pltpu.VMEM(strip, f32),
        pltpu.VMEM((rows + 2, width, extent_z), f32),
        pltpu.VMEM(strip, f32),
        pltpu.VMEM(home, f32),
        pltpu.VMEM((rows // fit, width, LANES), f32),
        pltpu.VMEM((block_y // fit, extent_x, LANES), f32),
        pltpu.VMEM((8, LANES), f32),
        pltpu.VMEM((grid, 8, LANES), f32),
        pltpu.VMEM((8, LANES), f32),
        pltpu.VMEM((shots * grid, 8, LANES), f32),
        dma((6,)), dma((4, one)), dma((4, one)), dma((2, one, chunks)), dma((2, one, chunks)),
        dma((steps + 1, 2)), dma((steps + 1, 2)), dma((steps + 1, 2)), dma((steps + 1, 2)), dma((4, 2)), dma((4, 2)),
        dma((shots - 1,)), dma((shots - 1,)), dma((shots - 1,)), dma((shots - 1,)),
        dma((across, chunks)), dma((one, chunks)), dma((across,)), dma((one,)),
        dma((grid - 1,)), dma((grid - 1,)), dma((shots * grid - 1,)), dma((shots * grid - 1,)),
    ]
    vmem, smem = pl.BlockSpec(memory_space=pltpu.VMEM), pl.BlockSpec(memory_space=pltpu.SMEM)
    dn, rec, stats, totals = pl.pallas_call(
        functools.partial(kernel, (shots, across, along, steps, fit, chunks)),
        out_shape=(
            jax.ShapeDtypeStruct(home, f32),
            jax.ShapeDtypeStruct((block_y // fit, extent_x, LANES), f32),
            jax.ShapeDtypeStruct((8, LANES), f32),
            jax.ShapeDtypeStruct((8, LANES), f32),
        ),
        in_specs=[smem, smem] + [vmem] * 8,
        out_specs=(vmem,) * 4,
        scratch_shapes=scratch,
        compiler_params=pltpu.CompilerParams(has_side_effects=True, vmem_limit_bytes=60 * 1024 * 1024),
        name="iteration",
    )(
        source_cell, wavelet, turned(state_now[0]), turned(state_prev[0]), turned(courant_sq),
        turned(direction), turned(prev_gradient), packed, live_lanes, rr,
    )
    sums = jnp.sum(stats, axis=1)
    ends = jnp.sum(totals, axis=1)
    beta = (sums[0] - sums[1]) / sums[2]
    slope = sums[0] + beta * sums[3]
    step = slope / ends[0]
    direction_next = turned(dn)
    image_next = reflectivity + step * direction_next
    rec = rec.reshape(block_y // fit, extent_x, fit, pitch)[..., :steps]
    records = jnp.transpose(rec, (3, 1, 0, 2)).reshape(steps, extent_x, block_y)
    residual_next = residual - step * records[None]
    entries = float(residual.size * shots * grid)
    misfit = ends[2] - 2.0 * step * ends[1] + step * step * ends[0]
    return image_next, direction_next, residual_next, 0.5 * misfit / entries


def solution(mesh):
    field, flat = P("shot", "gx", "gy", None), P("gx", "gy", None)
    traces = P("shot", None, "gx", "gy")
    return jax.shard_map(
        on_device,
        mesh=mesh,
        in_specs=(
            field, field, flat, flat, flat, flat, traces,
            P("shot", "gx", "gy"), P("shot", None), P("shot", None), P("shot"),
        ),
        out_specs=(flat, flat, traces, P()),
        check_vma=False,
    )
```
